256 devices in a mesh: pgroup: 32 (over y, x, core), tile: 8 (over z).
Axes of the slice: x: 4, y: 4, z: 8, core: 2. Of those that a mesh axis runs over, the one named last changes fastest.
Arguments:
- images: float32 [512, 256, 2048], P(('pgroup', 'tile')), may hold values from -6 to 6
- beams: float32 [512, 256, 2048], P(('pgroup', 'tile')), may hold values from 0.2 to 1
- row_block: int32 [512], P(('pgroup', 'tile')), may hold values from 0 to 30, as said below
- col_block: int32 [512], P(('pgroup', 'tile')), may hold values from 0 to 16
- band: int32 [512, 2], P(('pgroup', 'tile')), may hold values from 0 to 3
- row_frac: float32 [512], P(('pgroup', 'tile')), may hold values from 0.05 to 0.95
- col_frac: float32 [512], P(('pgroup', 'tile')), may hold values from 0.05 to 0.95
Outputs:
- numer: float32 [4096, 4096], P('tile', 'pgroup')
- weight: float32 [4096, 4096], P('tile', 'pgroup')
- normalised: float32 [4096, 4096], P('tile', 'pgroup')
The draws below stay inside these ranges and needn't reach their ends.
Inputs may be any that keep to these rules, and one draw needn't show every extreme that they name: With t = (p // 2) mod 8, row_block[p] - 4 t lies in 0 to 2, and the largest value is taken in every draw.
All inputs are finite; a program needn't handle non-finite values.
Results may differ from the reference program's by a relative error of at most 0.00002.
Values sent between devices are 32-bit elements; how exact they have to be, the bound alone decides.
No kernel may reach another device: no remote copies, remote signals or barrier semaphores. Data moves between devices by JAX's collectives and lax.ppermute only.
A program may use at most 128 MiB of HBM per device.

```python
import math
import jax
import jax.numpy as jnp
from jax import lax

W = 2048
IMG_ROWS = 256
IMG_BLOCKS = 2
PTS_DEV = 2
POINTINGS = 512
TILE_BLOCKS = 4
SKY_ROWS = 4096
SKY_COLS = 4096
HALO = 4
N_TILE = 8


def draw_row_block(key, part):
    pointing = jnp.arange(POINTINGS, dtype=jnp.int32)
    owner = pointing // PTS_DEV % N_TILE
    offset = jax.random.randint(key, (POINTINGS,), 0, TILE_BLOCKS - IMG_BLOCKS + 1, dtype=jnp.int32)
    offset = offset.at[0].set(TILE_BLOCKS - IMG_BLOCKS)
    return owner * TILE_BLOCKS + offset


def place_ends(array, own_key, low, high):
    index_at = [jax.random.randint(jax.random.fold_in(own_key, axis), (), 0, length) for axis, length in enumerate(array.shape)]
    widest = array.shape.index(max(array.shape))
    next_to = index_at[:widest] + [(index_at[widest] + 1) % array.shape[widest]] + index_at[widest + 1:]
    return array.at[tuple(index_at)].set(low).at[tuple(next_to)].set(high)


def level_of(own_key, shape, shards, least, largest):
    factor_of = 1.0
    for dim, blocks in shards:
        draws = jax.random.uniform(jax.random.fold_in(jax.random.fold_in(own_key, 6), dim), (blocks,), jnp.float32, least / len(shards), largest / len(shards))
        factor_of = factor_of * jnp.repeat(jnp.exp(draws), shape[dim] // blocks).reshape((-1,) + (1,) * (len(shape) - 1 - dim))
    return factor_of


def centred(rng, dims, width, reach, cuts=(), kind=jnp.bfloat16):
    level = level_of(rng, dims, cuts, -0.22, 0.18) if cuts else 1.0
    entries = jax.random.normal(rng, dims, jnp.float32) * width * level
    return jnp.minimum(jnp.maximum(entries, -reach), reach).astype(kind)


def setup_inputs(seed: int = 0) -> dict:
    key_list = jax.random.split(jax.random.key(seed), 8)
    return {
        "images": centred(key_list[0], (POINTINGS, IMG_ROWS, W), 1.0, 6.0, ((0, 256),), jnp.float32),
        "beams": jnp.clip(jnp.exp(math.log(1.0) - 1.609438 * jax.random.uniform(key_list[1], (POINTINGS, IMG_ROWS, W), jnp.float32) ** level_of(key_list[1], (POINTINGS, IMG_ROWS, W), ((0, 256),), -0.2, 0.2)), 0.2, 1.0),
        "row_block": draw_row_block(jax.random.fold_in(key_list[7], 71), 0),
        "col_block": place_ends(jax.random.randint(key_list[3], (POINTINGS,), 0, (SKY_COLS - W) // 128 + 1), jax.random.fold_in(key_list[3], 1), 0, ((SKY_COLS - W) // 128 + 1) - 1).astype(jnp.int32),
        "band": place_ends(jax.random.randint(key_list[4], (POINTINGS, IMG_BLOCKS), 0, HALO), jax.random.fold_in(key_list[4], 1), 0, HALO - 1).astype(jnp.int32),
        "row_frac": jnp.clip(0.05 + 0.9 * jax.random.uniform(key_list[5], (POINTINGS,), jnp.float32) ** level_of(key_list[5], (POINTINGS,), ((0, 256),), -0.2, 0.2), 0.05, 0.95),
        "col_frac": jnp.clip(0.05 + 0.9 * jax.random.uniform(key_list[6], (POINTINGS,), jnp.float32) ** level_of(key_list[6], (POINTINGS,), ((0, 256),), -0.2, 0.2), 0.05, 0.95),
    }


def contribution(image_block, beam_block, shift, row_f, col_f):
    stacked = jnp.stack([beam_block * image_block, beam_block * beam_block])
    moved = jnp.concatenate([jnp.zeros_like(stacked[:, :, :1]), stacked[:, :, :-1]], axis=2)
    banded = (1.0 - col_f) * stacked + col_f * moved
    empty = jnp.zeros((2, 128 + HALO, banded.shape[2]), jnp.float32)
    zero = jnp.int32(0)
    first = lax.dynamic_update_slice(empty, (1.0 - row_f) * banded, (zero, shift.astype(jnp.int32), zero))
    second = lax.dynamic_update_slice(empty, row_f * banded, (zero, (shift + 1).astype(jnp.int32), zero))
    return first + second


def reference(images, beams, row_block, col_block, band, row_frac, col_frac):
    canvas = jnp.zeros((2, SKY_ROWS + 128 + HALO, SKY_COLS), jnp.float32)

    def visit(index, canvas):
        for block in range(IMG_BLOCKS):
            image_block = lax.dynamic_slice_in_dim(images[index], block * 128, 128, 0)
            beam_block = lax.dynamic_slice_in_dim(beams[index], block * 128, 128, 0)
            piece = contribution(image_block, beam_block, band[index, block], row_frac[index], col_frac[index])
            row_start = ((row_block[index] + block) * 128).astype(jnp.int32)
            col_start = (col_block[index] * 128).astype(jnp.int32)
            zero = jnp.int32(0)
            old = lax.dynamic_slice(canvas, (zero, row_start, col_start), piece.shape)
            canvas = lax.dynamic_update_slice(canvas, old + piece, (zero, row_start, col_start))
        return canvas

    canvas = lax.fori_loop(0, POINTINGS, visit, canvas)
    numer = canvas[0, :SKY_ROWS]
    weight = canvas[1, :SKY_ROWS]
    normalised = numer / jnp.maximum(weight, 0.05)
    return numer, weight, normalised
```

```python
import functools

import jax
import jax.numpy as jnp
from jax import lax
from jax.experimental import pallas as pl
from jax.experimental.pallas import tpu as pltpu
from jax.sharding import PartitionSpec as P

SIDE = 4
N_TILE = 8
LANES = 128
OWN_ROWS = 512
IMG_ROWS = 256
IMG_COLS = 16
SKY_COLS = 32
HALO = 8
STRIP = 64


def place():
    group = lax.axis_index("pgroup")
    return group // 8, (group // 2) % 4, group % 2


def product_strip(image, beam, core, g):
    first = lax.broadcasted_iota(jnp.int32, image.shape, 1) == 0
    results = []
    for factor in (jnp.where(core == 0, image, beam), jnp.where(core == 0, beam, image)):
        product = factor * beam
        moved = jnp.where(first, 0.0, pltpu.roll(product, 1, 1))
        results.append((1.0 - g) * product + g * moved)
    return results


def split_columns(block):
    return [block[:, j * LANES : (j + 1) * LANES] for j in range(IMG_COLS)]


def lay_edges(tile, f, s):
    row = lax.broadcasted_iota(jnp.int32, (8, LANES), 0)
    near = (1.0 - f) * pltpu.roll(tile, s, 0)
    far = f * pltpu.roll(tile, s + 1, 0)
    return row, near, far


def head_of(tile, f, s):
    row, near, far = lay_edges(tile, f, s)
    return jnp.where(row >= s, near, 0.0) + jnp.where(row >= s + 1, far, 0.0)


def tail_of(tile, f, s):
    row, near, far = lay_edges(tile, f, s)
    return jnp.where(row < s, near, 0.0) + jnp.where(row < s + 1, far, 0.0)


def product_kernel(which, col_frac, images, beams, keep, send):
    core = lax.axis_index("pgroup") % 2
    g = col_frac[which]

    def strip(k, carry):
        rows = pl.ds(pl.multiple_of(k * 8, 8), 8)
        kept, sent = product_strip(images[0, rows, :], beams[0, rows, :], core, g)
        for j, piece in enumerate(split_columns(kept)):
            keep[j, rows, :] = piece
        for j, piece in enumerate(split_columns(sent)):
            send[j, rows, :] = piece
        return carry

    lax.fori_loop(0, STRIP // 8, strip, 0, unroll=True)


def products(which, col_frac, images, beams):
    piece = pl.BlockSpec((1, STRIP, IMG_COLS * LANES), lambda i: (which, i, 0))
    out = pl.BlockSpec((IMG_COLS, STRIP, LANES), lambda i: (0, i, 0))
    shape = jax.ShapeDtypeStruct((IMG_COLS, IMG_ROWS, LANES), jnp.float32)
    return pl.pallas_call(
        functools.partial(product_kernel, which),
        grid=(IMG_ROWS // STRIP,),
        in_specs=[pl.BlockSpec(memory_space=pltpu.SMEM), piece, piece],
        out_specs=[out, out],
        out_shape=[shape, shape],
        cost_estimate=pl.CostEstimate(flops=20_000_000, bytes_accessed=8 << 20, transcendentals=0),
        name=f"products{which}",
    )(col_frac, images, beams)


def pack_kernel(row_block, col_block, band, row_frac, packed):
    tile = lax.axis_index("tile")
    for p in range(2):
        packed[4 * p] = (row_block[p] - 4 * tile).astype(jnp.float32)
        packed[4 * p + 1] = col_block[p].astype(jnp.float32)
        packed[4 * p + 2] = band[p, 0].astype(jnp.float32)
        packed[4 * p + 3] = band[p, 1].astype(jnp.float32)
        packed[8 + p] = row_frac[p]


def pack(row_block, col_block, band, row_frac):
    smem = pl.BlockSpec(memory_space=pltpu.SMEM)
    return pl.pallas_call(
        pack_kernel,
        in_specs=[smem] * 4,
        out_specs=smem,
        out_shape=jax.ShapeDtypeStruct((16,), jnp.float32),
        name="pack",
    )(row_block, col_block, band, row_frac)


def halo_kernel(packed, keep0, keep1, send0, send1, same, cross):
    for out, sources in ((same, (keep0, keep1)), (cross, (send0, send1))):
        out[...] = jnp.zeros_like(out)
        for p, source in enumerate(sources):
            offset = packed[4 * p].astype(jnp.int32)
            column = packed[4 * p + 1].astype(jnp.int32)
            s = packed[4 * p + 3].astype(jnp.int32)
            f = packed[8 + p]

            @pl.when(offset == 2)
            def _():
                def piece(j, carry):
                    out[column + j] += tail_of(source[j], f, s)
                    return carry

                lax.fori_loop(0, IMG_COLS, piece, 0, unroll=4)


def halos(packed, keep, send):
    last = pl.BlockSpec((IMG_COLS, 8, LANES), lambda i: (0, IMG_ROWS // 8 - 1, 0))
    whole = pl.BlockSpec((SKY_COLS, HALO, LANES), lambda i: (0, 0, 0))
    shape = jax.ShapeDtypeStruct((SKY_COLS, HALO, LANES), jnp.float32)
    return pl.pallas_call(
        halo_kernel,
        grid=(1,),
        in_specs=[pl.BlockSpec(memory_space=pltpu.SMEM)] + [last] * 4,
        out_specs=[whole, whole],
        out_shape=[shape, shape],
        cost_estimate=pl.CostEstimate(flops=1_000_000, bytes_accessed=1 << 19, transcendentals=0),
        name="halos",
    )(packed, *keep, *send)


def sky_column(du, dv, cross):
    y, x, core = place()
    u, v = jnp.where(core == 0, x, y), jnp.where(core == 0, y, x)
    u, v = (u + du) % SIDE, (v + dv) % SIDE
    other = (core + cross) % 2
    return jnp.where(core == 0, 8 * v + 2 * u, 8 * u + 2 * v) + other


def assemble_kernel(du, mine, theirs, *refs):
    sources, borders, outs = refs[:8], refs[8:12], refs[12:]
    dv = pl.program_id(0)
    for cross in range(2):
        out = outs[cross]
        column = sky_column(du, dv, cross)
        out[...] = jnp.zeros_like(out)
        out[0, 0:HALO, :] = borders[2 * cross][0] + borders[2 * cross + 1][0]
        for p in range(4):
            packed = (mine, theirs)[p // 2]
            source = sources[4 * cross + p]
            at = 4 * (p % 2)
            start = packed[at + 1].astype(jnp.int32)
            offset = packed[at].astype(jnp.int32)
            f = packed[8 + p % 2]
            shifts = [packed[at + 2 + b].astype(jnp.int32) for b in range(2)]

            @pl.when((column >= start) & (column < start + IMG_COLS))
            def _():
                for b in range(2):
                    s = shifts[b]
                    base = b * 128
                    top = pl.multiple_of((offset + b) * 128, 128)
                    out[0, pl.ds(top, 8), :] += head_of(source[0, base : base + 8, :], f, s)
                    inner = pl.ds(pl.multiple_of(top + 8, 8), 120)
                    out[0, inner, :] += (1.0 - f) * source[0, pl.ds(base + 8 - s, 120), :] + f * source[0, pl.ds(base + 7 - s, 120), :]
                    last = source[0, base + 120 : base + 128, :]

                    @pl.when(offset + b < 3)
                    def _():
                        out[0, pl.ds(pl.multiple_of(top + 128, 128), 8), :] += tail_of(last, f, s)


def assemble(du, mine, theirs, keep, received, borders):
    def source_spec(p, cross):
        def index(dv, own, other):
            start = (own, other)[p // 2][4 * (p % 2) + 1].astype(jnp.int32)
            return jnp.clip(sky_column(du, dv, cross) - start, 0, IMG_COLS - 1), 0, 0

        return pl.BlockSpec((1, IMG_ROWS, LANES), index)

    def border_spec(cross):
        return pl.BlockSpec((1, HALO, LANES), lambda dv, own, other: (sky_column(du, dv, cross), 0, 0))

    out = pl.BlockSpec((1, OWN_ROWS, LANES), lambda dv, own, other: (dv, 0, 0))
    shape = jax.ShapeDtypeStruct((SIDE, OWN_ROWS, LANES), jnp.float32)
    return pl.pallas_call(
        functools.partial(assemble_kernel, du),
        grid_spec=pltpu.PrefetchScalarGridSpec(
            num_scalar_prefetch=2,
            grid=(SIDE,),
            in_specs=[source_spec(p, cross) for cross in range(2) for p in range(4)]
            + [border_spec(cross) for cross in range(2) for _ in range(2)],
            out_specs=[out, out],
        ),
        out_shape=[shape, shape],
        cost_estimate=pl.CostEstimate(flops=10_000_000, bytes_accessed=4 << 20, transcendentals=0),
        name=f"assemble{du}",
    )(mine, theirs, *keep, *received, *keep, *received, *borders, *borders)


def moves():
    chips = [(y, x) for y in range(SIDE) for x in range(SIDE)]

    def index(y, x, core):
        return 8 * (y % SIDE) + 2 * (x % SIDE) + core

    def along(core, y, x, first, step):
        on_x = (core == 0) == first
        return (y, x + step) if on_x else (y + step, x)

    def route(first, step, cross):
        return [
            (index(y, x, core), index(*along(core, y, x, first, step), (core + cross) % 2))
            for y, x in chips
            for core in range(2)
        ]

    return route


ROUTE = moves()


def send_first(array, step):
    return lax.ppermute(array, "pgroup", ROUTE(True, step, 0))


def send_second(array, step, cross):
    return lax.ppermute(array, "pgroup", ROUTE(False, step, cross))


def send_partner(array):
    return lax.ppermute(array, "pgroup", ROUTE(True, 0, 1))


def send_border(array, cross):
    pairs = []
    for source, target in ROUTE(True, 0, cross):
        pairs += [(source * N_TILE + tile, target * N_TILE + tile + 1) for tile in range(N_TILE - 1)]
    return lax.ppermute(array, ("pgroup", "tile"), pairs)


def body(images, beams, row_block, col_block, band, row_frac, col_frac):
    mine = pack(row_block, col_block, band, row_frac)
    theirs = send_partner(mine)
    keep0, send0 = products(0, col_frac, images, beams)
    got0 = send_partner(send0)
    keep1, send1 = products(1, col_frac, images, beams)
    got1 = send_partner(send1)
    keep, got = (keep0, keep1), (got0, got1)
    same, cross = halos(mine, keep, (send0, send1))
    borders = (send_border(same, 0), send_border(cross, 1))
    blocks = functools.partial(assemble, mine=mine, theirs=theirs, keep=keep, received=got, borders=borders)

    p2, q2 = blocks(2)
    relay_up, relay_down = send_first(p2, 1), send_first(q2, -1)
    p1, q1 = blocks(1)
    direct_up = send_first(q1, 1)
    p3, q3 = blocks(3)
    direct_down = send_first(p3, -1)
    p0, q0 = blocks(0)
    joined_up = send_first(p1 + relay_up, 1)
    joined_down = send_first(q3 + relay_down, -1)

    def own_p(dv):
        return p0[dv] + joined_up[dv] + direct_down[dv]

    def own_q(dv):
        return q0[dv] + joined_down[dv] + direct_up[dv]

    passed_up = send_second(own_p(2), 1, 0)
    passed_down = send_second(own_q(2), -1, 0)
    cross_up = send_second(own_q(1), 1, 1)
    home_down = send_second(own_p(3), -1, 0)
    partner = send_partner(own_q(0))
    home_up = send_second(own_p(1) + passed_up, 1, 0)
    cross_down = send_second(own_q(3) + passed_down, -1, 1)
    home = own_p(0) + home_down + home_up
    away = partner + cross_up + cross_down
    on_numer = lax.axis_index("pgroup") % 2 == 0
    numer = jnp.where(on_numer, home, away)
    weight = jnp.where(on_numer, away, home)
    return numer, weight, numer / jnp.maximum(weight, 0.05)


def solution(mesh):
    return jax.shard_map(
        body,
        mesh=mesh,
        in_specs=(
            P(("pgroup", "tile"), None, None),
            P(("pgroup", "tile"), None, None),
            P(("pgroup", "tile")),
            P(("pgroup", "tile")),
            P(("pgroup", "tile"), None),
            P(("pgroup", "tile")),
            P(("pgroup", "tile")),
        ),
        out_specs=(P("tile", "pgroup"), P("tile", "pgroup"), P("tile", "pgroup")),
        check_vma=False,
    )
```
